32 devices in a mesh: image: 4 (over y, x), band: 2 (over core), ga: 4 (over z).
Axes of the slice: x: 2, y: 2, z: 4, core: 2. Of those that a mesh axis runs over, the one named last changes fastest.
Arguments:
- wave_coeffs: bfloat16 [4, 64, 2, 262144], P('image', 'band', None, 'ga'), may hold values from -6 to 6
- occupation: float32 [4, 64], P('image', 'band'), may hold values from 0.003125 to 0.0625
- form_factor: float32 [4, 8, 262144], P(None, None, 'ga'), may hold values from -0.005859375 to 0.005859375
- g_vectors: float32 [3, 262144], P(None, 'ga'), may hold values from -2 to 2
- species: int32 [64], replicated, may hold values from 0 to 3
- proj_count: int32 [4], replicated, may hold values from 1 to 8, as said below
- coupling: float32 [4, 8], replicated, may hold values from 0.5 to 2.5
- positions: float32 [4, 3, 64], P('image'), may hold values from -5.4 to 29.4, as said below
- energy_rest: float32 [4], P('image'), may hold values from -8 to 8
- force_rest: float32 [4, 3, 64], P('image'), may hold values from -6 to 6
- end_positions: float32 [2, 3, 64], replicated, may hold values from -5.4 to 29.4, as said below
- end_energy: float32 [2], replicated, may hold values from -8 to 8
- climb_index: int32 [1], replicated, may hold values from 0 to 3
- tangent_kind: int32 [4], P('image'), may hold values from 0 to 3
Outputs:
- neb_force: float32 [4, 3, 64], P('image')
- energy: float32 [4], P('image')
The draws below stay inside these ranges and needn't reach their ends.
Inputs may be any that keep to these rules, and one draw needn't show every extreme that they name: `proj_count`: each species has between 1 and 8 live projector slots, and some species has exactly 8. `positions`: atom coordinates in bohr. `end_positions`: atom coordinates in bohr.
All inputs are finite; a program needn't handle non-finite values.
Results may differ from the reference program's by a relative error of at most 0.0003.
The reference program's roundings to bfloat16 on the way (of `projector` and `stacked`) count: a program that leaves them out, or rounds other values in their place, can miss the bound.
Values sent between devices are 32-bit elements; how exact they have to be, the bound alone decides.
No kernel may reach another device: no remote copies, remote signals or barrier semaphores. Data moves between devices by JAX's collectives and lax.ppermute only.
A program may use at most 128 MiB of HBM per device.

```python
import jax
import jax.numpy as jnp
from jax import lax

NG = 262144
ATOMS = 64
PMAX = 8
SPECIES = 4
IMG = 4
BANDS = 64
N_GA = 4


def chain_path(key):
    base_key = jax.random.fold_in(key, 11)
    step_key = jax.random.fold_in(key, 12)
    base = jax.random.uniform(base_key, (3, ATOMS), jnp.float32, 0.0, 24.0)
    steps = 0.3 * jnp.clip(jax.random.normal(step_key, (IMG + 2, 3, ATOMS), jnp.float32), -3.0, 3.0)
    return base[None, :, :] + jnp.cumsum(steps, axis=0)


def draw_positions(key, part):
    return chain_path(key)[1:IMG + 1]


def draw_end_positions(key, part):
    path = chain_path(key)
    return jnp.stack([path[0], path[IMG + 1]], axis=0)


def draw_proj_count(key, part):
    counts = jax.random.randint(jax.random.fold_in(key, 21), (SPECIES,), 1, PMAX + 1, jnp.int32)
    filled = jax.random.randint(jax.random.fold_in(key, 22), (), 0, SPECIES, jnp.int32)
    return jnp.where(jnp.arange(SPECIES, dtype=jnp.int32) == filled, PMAX, counts).astype(jnp.int32)


def place_ends(drawn, rng, smallest, high):
    shape = drawn.shape
    spot = [jax.random.randint(jax.random.fold_in(rng, axis), (), 0, shape[axis]) for axis in range(len(shape))]
    drawn = drawn.at[tuple(spot)].set(smallest)
    longest = shape.index(max(shape))
    spot[longest] = (spot[longest] + 1) % shape[longest]
    return drawn.at[tuple(spot)].set(high)


def levels(stream_key, extent, cuts, low, top_value):
    loudness = 1.0
    for dim, blocks in cuts:
        steps = jax.random.uniform(jax.random.fold_in(jax.random.fold_in(stream_key, 6), dim), (blocks,), jnp.float32, low / len(cuts), top_value / len(cuts))
        loudness = loudness * jnp.repeat(jnp.exp(steps), extent[dim] // blocks).reshape((-1,) + (1,) * (len(extent) - 1 - dim))
    return loudness


def centred(stream_key, dims, deviation, limit, cuts=(), kind=jnp.bfloat16):
    array = jax.random.normal(stream_key, dims, jnp.float32) * deviation
    if len(cuts) > 0:
        array = levels(stream_key, dims, cuts, -0.22, 0.18) * array
    return jnp.clip(array, min=-limit, max=limit).astype(kind)


def setup_inputs(seed: int = 0) -> dict:
    key_of = jax.random.split(jax.random.key(seed), 15)
    return {
        "wave_coeffs": centred(key_of[0], (IMG, BANDS, 2, NG), 1.0, 6.0, ((0, 4), (1, 2), (3, 4))),
        "occupation": jnp.clip(0.003125 + 0.059375 * jax.random.uniform(key_of[1], (IMG, BANDS), jnp.float32) ** levels(key_of[1], (IMG, BANDS), ((0, 4), (1, 2)), -0.2, 0.2), 0.003125, 0.0625),
        "form_factor": centred(key_of[2], (SPECIES, PMAX, NG), (4 * NG) ** -0.5, 0.005859375, ((2, 4),), jnp.float32),
        "g_vectors": jnp.clip(jax.random.uniform(key_of[3], (3, NG), jnp.float32, -2.0, 2.0) * levels(key_of[3], (3, NG), ((1, 4),), -0.4, 0.0), -2.0, 2.0),
        "species": place_ends(jax.random.randint(key_of[4], (ATOMS,), 0, SPECIES), jax.random.fold_in(key_of[4], 1), 0, SPECIES - 1).astype(jnp.int32),
        "proj_count": draw_proj_count(jax.random.fold_in(key_of[14], 71), 0),
        "coupling": jnp.clip(jax.random.uniform(key_of[6], (SPECIES, PMAX), jnp.float32, 0.5, 2.5), 0.5, 2.5),
        "positions": draw_positions(jax.random.fold_in(key_of[14], 71), 0),
        "energy_rest": centred(key_of[8], (IMG,), 2.0, 8.0, ((0, 4),), jnp.float32),
        "force_rest": centred(key_of[9], (IMG, 3, ATOMS), 1.0, 6.0, ((0, 4),), jnp.float32),
        "end_positions": draw_end_positions(jax.random.fold_in(key_of[14], 71), 0),
        "end_energy": centred(key_of[11], (2,), 2.0, 8.0, (), jnp.float32),
        "climb_index": jax.random.randint(key_of[12], (1,), 0, IMG).astype(jnp.int32),
        "tangent_kind": place_ends(jax.random.randint(key_of[13], (IMG,), 0, 4), jax.random.fold_in(key_of[13], 1), 0, 3).astype(jnp.int32),
    }


spring_constant = 5.0

def atom_tables(species, proj_count, coupling):
    is_species = (species[:, None] == jnp.arange(SPECIES)[None, :]).astype(jnp.float32)
    is_live = (jnp.arange(PMAX)[None, :] < proj_count[:, None]).astype(jnp.float32)
    species_mask = is_species[:, :, None] * is_live[None, :, :]
    strength = lax.optimization_barrier(jnp.sum(species_mask * coupling[None, :, :], axis=1))
    return (species_mask, strength)

def projectors(atom_pos, species_mask, form_factor, g_vectors):
    phases = atom_pos[0][:, None] * g_vectors[0][None, :]
    phases = phases + atom_pos[1][:, None] * g_vectors[1][None, :]
    phases = phases + atom_pos[2][:, None] * g_vectors[2][None, :]
    cosine = jnp.cos(phases)
    sine_part = jnp.sin(phases)
    radial = species_mask[:, 0, :, None] * form_factor[0][None, :, :]
    for spec_num in range(1, SPECIES):
        radial = radial + species_mask[:, spec_num, :, None] * form_factor[spec_num][None, :, :]
    real_part = radial * cosine[:, None, :]
    imag_part = -radial * sine_part[:, None, :]
    joined = jnp.concatenate([real_part, imag_part], axis=-1).astype(jnp.bfloat16)
    return joined.reshape(joined.shape[0] * joined.shape[1], joined.shape[2])

def stack_waves(waves_here, g_vectors):
    band_count = waves_here.shape[0]
    real_part = waves_here[:, 0, :].astype(jnp.float32)
    imag_part = waves_here[:, 1, :].astype(jnp.float32)
    pieces = [waves_here.reshape(band_count, 2 * waves_here.shape[2])]
    for axis_num in range(3):
        direction = g_vectors[axis_num][None, :]
        pieces.append(jnp.concatenate([-direction * imag_part, direction * real_part], axis=-1).astype(jnp.bfloat16))
    return jnp.concatenate(pieces, axis=0)

def contract(projector, stacked):
    return 2.0 * lax.dot_general(projector, stacked, (((1,), (1,)), ((), ())), preferred_element_type=jnp.float32)

def nonlocal_terms(proj_sums, occupied, strength):
    band_count = occupied.shape[0]
    atom_count = strength.shape[0]
    intersect = proj_sums[:, :band_count]
    weighted = intersect * occupied[None, :]
    energy_part = jnp.sum(strength.reshape(-1) * lax.optimization_barrier(jnp.sum(weighted * intersect, axis=1)))
    forces = []
    for axis_num in range(3):
        slope = proj_sums[:, (axis_num + 1) * band_count:(axis_num + 2) * band_count]
        per_row = lax.optimization_barrier(jnp.sum(weighted * slope, axis=1)).reshape(atom_count, PMAX)
        forces.append(-2.0 * lax.optimization_barrier(jnp.sum(strength * per_row, axis=1)))
    return (energy_part, jnp.stack(forces, axis=0))

def neb_project(force, here, prev_pos, next_pos, energy, prev_energy, next_energy, tangent_kind, is_climb):
    to_next = next_pos - here
    from_prev = here - prev_pos
    rise_next = jnp.abs(next_energy - energy)
    rise_prev = jnp.abs(prev_energy - energy)
    larger = jnp.maximum(rise_next, rise_prev)
    smaller = jnp.minimum(rise_next, rise_prev)
    rising = next_energy > prev_energy
    weight_next = 1.0 + jnp.where(rising, larger, smaller)
    weight_prev = 1.0 + jnp.where(rising, smaller, larger)
    stiff_next = spring_constant * (1.0 + jax.nn.sigmoid(0.5 * (next_energy + energy)))
    stiff_prev = spring_constant * (1.0 + jax.nn.sigmoid(0.5 * (prev_energy + energy)))
    length_next = jnp.sqrt(lax.optimization_barrier(jnp.sum(to_next * to_next, axis=(1, 2))) + 1.0)
    length_prev = jnp.sqrt(lax.optimization_barrier(jnp.sum(from_prev * from_prev, axis=(1, 2))) + 1.0)
    upwind = weight_next[:, None, None] * to_next + weight_prev[:, None, None] * from_prev
    forward = to_next / length_next[:, None, None]
    backward = from_prev / length_prev[:, None, None]
    kind = tangent_kind[:, None, None]
    tangent = jnp.where(kind == 0, upwind, jnp.where(kind == 1, forward + backward, jnp.where(kind == 2, forward, backward)))
    unit_tangent = tangent / jnp.sqrt(lax.optimization_barrier(jnp.sum(tangent * tangent, axis=(1, 2))) + 1.0)[:, None, None]
    along = lax.optimization_barrier(jnp.sum(force * unit_tangent, axis=(1, 2)))[:, None, None]
    climbing = force - 2.0 * along * unit_tangent
    regular = force - along * unit_tangent + (stiff_next * length_next - stiff_prev * length_prev)[:, None, None] * unit_tangent
    return jnp.where(is_climb[:, None, None], climbing, regular)

def reference(wave_coeffs, occupation, form_factor, g_vectors, species, proj_count, coupling, positions, energy_rest, force_rest, end_positions, end_energy, climb_index, tangent_kind):
    species_mask, strength = atom_tables(species, proj_count, coupling)
    block_len = NG // N_GA
    energies = []
    forces = []
    for image_num in range(IMG):
        waves_image = wave_coeffs[image_num]
        atom_pos = positions[image_num]

        def accumulate(block_num, total):
            start = (block_num * block_len).astype(jnp.int32)
            waves_block = lax.dynamic_slice_in_dim(waves_image, start, block_len, 2)
            form_block = lax.dynamic_slice_in_dim(form_factor, start, block_len, 2)
            g_block = lax.dynamic_slice_in_dim(g_vectors, start, block_len, 1)
            stacked = stack_waves(waves_block, g_block)
            projector = projectors(atom_pos, species_mask, form_block, g_block)
            return total + contract(projector, stacked)
        initial = jnp.zeros((ATOMS * PMAX, 4 * BANDS), jnp.float32)
        proj_sums = lax.fori_loop(0, N_GA, accumulate, initial)
        energy_part, force_part = nonlocal_terms(proj_sums, occupation[image_num], strength)
        energies.append(energy_part)
        forces.append(force_part)
    energy = energy_rest + jnp.stack(energies)
    force = force_rest + jnp.stack(forces, axis=0)
    chain_pos = jnp.concatenate([end_positions[:1], positions, end_positions[1:]], axis=0)
    chain_energy = jnp.concatenate([end_energy[:1], energy, end_energy[1:]], axis=0)
    is_climb = jnp.arange(IMG, dtype=jnp.int32) == climb_index[0]
    neb_force = neb_project(force, positions, chain_pos[:-2], chain_pos[2:], energy, chain_energy[:-2], chain_energy[2:], tangent_kind, is_climb)
    return (neb_force, energy)
```

```python
import functools

import jax
import jax.numpy as jnp
from jax import lax
from jax.experimental import pallas as pl
from jax.experimental.pallas import tpu as pltpu
from jax.sharding import PartitionSpec as P

ATOMS = 64
PMAX = 8
SPECIES = 4


spring_constant = 5.0


S2=(7.07106765e-01, -2.94627488e-02, 3.68265567e-04, -2.18770204e-06, 7.15483753e-09)
C2=(1.41421350e+00, -1.76776359e-01, 3.68257460e-03, -3.06124985e-05, 1.27899789e-07)
P1=6.283203125; P2=-1.781782029e-05; IT=0.15915494309189535

def cos_negsin(x):
    k = jnp.round(x*IT)
    r = (x - k*P1) - k*P2
    y = r*r
    s = S2[4]
    for q in S2[3::-1]: s = s*y + q
    s = s*r
    c = C2[4]
    for q in C2[3::-1]: c = c*y + q
    return 1.0 - s*s, -(s*c)

def body_trig(w_ref, ff_ref, g_ref, pos_ref, live_ref, cs, sn, fm, stk, off, gc, atoms, pmax, nspec, bands):
    for j in range(gc//128):
        sl = pl.ds(off+128*j, 128); dl = pl.ds(128*j,128); dl2 = pl.ds(gc+128*j,128)
        g = [g_ref[c:c+1, sl] for c in range(3)]
        for s in range(nspec):
            fm[j, s] = ff_ref[s, :, sl]*live_ref[s]
        for a in range(0, atoms, 8):
            ph = pos_ref[0, a:a+8, :]*g[0]
            ph = ph + pos_ref[1, a:a+8, :]*g[1]
            ph = ph + pos_ref[2, a:a+8, :]*g[2]
            co, ns = cos_negsin(ph)
            cs[j, a:a+8, :] = co
            sn[j, a:a+8, :] = ns
        for n in range(0, bands, 16):
            ub = w_ref[n:n+16, sl]; vb = w_ref[bands+n:bands+n+16, sl]
            stk[n:n+16, dl] = ub; stk[n:n+16, dl2] = vb
            u = ub.astype(jnp.float32); v = vb.astype(jnp.float32)
            for c in range(3):
                stk[(c+1)*bands+n:(c+1)*bands+n+16, dl] = (v*(-g[c])).astype(jnp.bfloat16)
                stk[(c+1)*bands+n:(c+1)*bands+n+16, dl2] = (u*g[c]).astype(jnp.bfloat16)

def body_mm(sp, acc, cs, sn, fm, stk, gc, atoms, pmax, rb):
    for r0 in range(0, atoms*pmax, rb):
        rows=[]
        for a in range(r0//pmax, (r0+rb)//pmax, 16//pmax):
            half=[]
            for t in (cs, sn):
                for j in range(gc//128):
                    half.append(jnp.concatenate([fm[j, sp[b]]*t[j, pl.ds(b, pmax, stride=0), :] for b in range(a, a+16//pmax)],0).astype(jnp.bfloat16))
            rows.append(jnp.concatenate(half,1))
        P = jnp.concatenate(rows,0)
        acc[r0:r0+rb, :] += lax.dot_general(P, stk[...], (((1,),(1,)),((),())), preferred_element_type=jnp.float32)

def kern2(sp, w_ref, ff_ref, g_ref, pos_ref, live_ref, acc, csA, snA, fmA, csB, snB, fmB, sA, sB, *, gc, nsub, dims, rb):
    i = pl.program_id(0)
    atoms,pmax,nspec,bands = dims
    @pl.when(i==0)
    def _():
        acc[...] = jnp.zeros_like(acc)
        for r in (csB, snB, fmB, sB): r[...] = jnp.zeros_like(r)
    gen = functools.partial(body_trig, w_ref, ff_ref, g_ref, pos_ref, live_ref)
    def step(t, _):
        base = pl.multiple_of(t*2*gc, 128)
        gen(csA, snA, fmA, sA, base, gc, *dims)
        body_mm(sp, acc, csB, snB, fmB, sB, gc, atoms, pmax, rb)
        gen(csB, snB, fmB, sB, base+gc, gc, *dims)
        body_mm(sp, acc, csA, snA, fmA, sA, gc, atoms, pmax, rb)
        return 0
    lax.fori_loop(0, nsub, step, 0)
    @pl.when(i==pl.num_programs(0)-1)
    def _():
        body_mm(sp, acc, csB, snB, fmB, sB, gc, atoms, pmax, rb)
        acc[...] = 2.0*acc[...]

def contract(sp, w, ff, g, posb, live, gc=1024, blk=4096, rb=256):
    nspec,pmax,G = ff.shape; atoms = posb.shape[1]; bands=w.shape[0]//2
    rows=atoms*pmax
    f32=jnp.float32; bf=jnp.bfloat16
    blk=min(blk, G); gc=min(gc, blk//2)
    return pl.pallas_call(
        functools.partial(kern2, gc=gc, nsub=blk//(2*gc), dims=(atoms,pmax,nspec,bands), rb=rb),
        grid=(G//blk,),
        out_shape=jax.ShapeDtypeStruct((rows,4*bands), f32),
        in_specs=[pl.BlockSpec(memory_space=pltpu.SMEM),
            pl.BlockSpec((2*bands,blk), lambda i:(0,i)),
            pl.BlockSpec((nspec,pmax,blk), lambda i:(0,0,i)),
            pl.BlockSpec((3,blk), lambda i:(0,i)),
            pl.BlockSpec((3,atoms,128), lambda i:(0,0,0)),
            pl.BlockSpec((nspec,pmax,128), lambda i:(0,0,0))],
        out_specs=pl.BlockSpec((rows,4*bands), lambda i:(0,0)),
        scratch_shapes=[pltpu.VMEM((gc//128,atoms,128),f32),pltpu.VMEM((gc//128,atoms,128),f32),pltpu.VMEM((gc//128,nspec,pmax,128),f32)]*2
          +[pltpu.VMEM((4*bands,2*gc),bf)]*2,
        compiler_params=pltpu.CompilerParams(dimension_semantics=("arbitrary",), vmem_limit_bytes=48*2**20),
        name="nl",
    )(sp, w, ff, g, posb, live)

def passed_along(array, axis, by):
    length = lax.axis_size(axis)
    pairs = [(i, i + by) for i in range(length) if 0 <= i + by < length]
    return lax.ppermute(array, axis, pairs)


def atom_tables(species, proj_count, coupling):
    is_species = (species[:, None] == jnp.arange(SPECIES)[None, :]).astype(jnp.float32)
    is_live = (jnp.arange(PMAX)[None, :] < proj_count[:, None]).astype(jnp.float32)
    species_mask = is_species[:, :, None] * is_live[None, :, :]
    strength = jnp.sum(species_mask * coupling[None, :, :], axis=1)
    return (species_mask, strength)


def nonlocal_terms(proj_sums, occupied, strength):
    band_count = occupied.shape[0]
    atom_count = strength.shape[0]
    intersect = proj_sums[:, :band_count]
    weighted = intersect * occupied[None, :]
    energy_part = jnp.sum(strength.reshape(-1) * jnp.sum(weighted * intersect, axis=1))
    forces = []
    for axis_num in range(3):
        slope = proj_sums[:, (axis_num + 1) * band_count : (axis_num + 2) * band_count]
        per_row = jnp.sum(weighted * slope, axis=1).reshape(atom_count, PMAX)
        forces.append(-2.0 * jnp.sum(strength * per_row, axis=1))
    return (energy_part, jnp.stack(forces, axis=0))


def neb_project(
    force, here, prev_pos, next_pos, energy, prev_energy, next_energy, tangent_kind, is_climb
):
    to_next = next_pos - here
    from_prev = here - prev_pos
    rise_next = jnp.abs(next_energy - energy)
    rise_prev = jnp.abs(prev_energy - energy)
    larger = jnp.maximum(rise_next, rise_prev)
    smaller = jnp.minimum(rise_next, rise_prev)
    rising = next_energy > prev_energy
    weight_next = 1.0 + jnp.where(rising, larger, smaller)
    weight_prev = 1.0 + jnp.where(rising, smaller, larger)
    stiff_next = spring_constant * (1.0 + jax.nn.sigmoid(0.5 * (next_energy + energy)))
    stiff_prev = spring_constant * (1.0 + jax.nn.sigmoid(0.5 * (prev_energy + energy)))
    length_next = jnp.sqrt(jnp.sum(to_next * to_next, axis=(1, 2)) + 1.0)
    length_prev = jnp.sqrt(jnp.sum(from_prev * from_prev, axis=(1, 2)) + 1.0)
    upwind = weight_next[:, None, None] * to_next + weight_prev[:, None, None] * from_prev
    forward = to_next / length_next[:, None, None]
    backward = from_prev / length_prev[:, None, None]
    kind = tangent_kind[:, None, None]
    tangent = jnp.where(
        kind == 0,
        upwind,
        jnp.where(kind == 1, forward + backward, jnp.where(kind == 2, forward, backward)),
    )
    unit_tangent = tangent / jnp.sqrt(jnp.sum(tangent * tangent, axis=(1, 2)) + 1.0)[:, None, None]
    along = jnp.sum(force * unit_tangent, axis=(1, 2))[:, None, None]
    climbing = force - 2.0 * along * unit_tangent
    regular = (
        force
        - along * unit_tangent
        + (stiff_next * length_next - stiff_prev * length_prev)[:, None, None] * unit_tangent
    )
    return jnp.where(is_climb[:, None, None], climbing, regular)


def swapped(array, axis, mask):
    pairs = [(i, i ^ mask) for i in range(lax.axis_size(axis))]
    return lax.ppermute(array, axis, pairs)


def summed(array, axis):
    size = lax.axis_size(axis)
    if size & (size - 1):
        return lax.psum(array, axis)
    mask = 1
    while mask < size:
        array = array + swapped(array, axis, mask)
        mask *= 2
    return array


def scattered_rows(rows, axis):
    size = lax.axis_size(axis)
    index = lax.axis_index(axis)
    if size & (size - 1):
        block = rows.shape[0] // size
        return lax.psum_scatter(rows, axis, scatter_dimension=0, tiled=True), index * block
    first = jnp.int32(0)
    mask = 1
    while mask < size:
        half = rows.shape[0] // 2
        bit = (index // mask) % 2
        kept = lax.dynamic_slice_in_dim(rows, bit * half, half, 0)
        sent = lax.dynamic_slice_in_dim(rows, (1 - bit) * half, half, 0)
        rows = kept + swapped(sent, axis, mask)
        first = first + bit * half
        mask *= 2
    return rows, first


def per_device(
    wave_coeffs,
    occupation,
    form_factor,
    g_vectors,
    species,
    proj_count,
    coupling,
    positions,
    energy_rest,
    force_rest,
    end_positions,
    end_energy,
    climb_index,
    tangent_kind,
):
    species_mask, strength = atom_tables(species, proj_count, coupling)
    prev_pos = passed_along(positions, "image", 1)
    next_pos = passed_along(positions, "image", -1)
    bands = wave_coeffs.shape[1]
    waves = wave_coeffs[0].transpose(1, 0, 2).reshape(2 * bands, wave_coeffs.shape[3])
    is_live = (jnp.arange(PMAX)[None, :] < proj_count[:, None]).astype(jnp.float32)
    sums = contract(
        species,
        waves,
        form_factor,
        g_vectors,
        jnp.broadcast_to(positions[0][:, :, None], (3, ATOMS, 128)),
        jnp.broadcast_to(is_live[:, :, None], (SPECIES, PMAX, 128)),
    )
    proj_sums, first_row = scattered_rows(sums, "ga")
    first_local = first_row // PMAX
    local_atoms = proj_sums.shape[0] // PMAX
    strength_part = lax.dynamic_slice_in_dim(strength, first_local, local_atoms, 0)
    energy_part, force_part = nonlocal_terms(proj_sums, occupation[0], strength_part)
    force_full = lax.dynamic_update_slice_in_dim(
        jnp.zeros((3, ATOMS), jnp.float32), force_part, first_local, 1
    )
    packed = jnp.concatenate(
        [force_full, jnp.full((1, ATOMS), energy_part, jnp.float32)], axis=0
    )
    packed = summed(summed(packed, "band"), "ga")
    energy = energy_rest + packed[3, :1]
    force = force_rest + packed[None, :3, :]
    image_index = lax.axis_index("image")
    image_count = lax.axis_size("image")
    prev_energy = passed_along(energy, "image", 1)
    next_energy = passed_along(energy, "image", -1)
    at_start = image_index == 0
    at_end = image_index == image_count - 1
    prev_pos = jnp.where(at_start, end_positions[:1], prev_pos)
    prev_energy = jnp.where(at_start, end_energy[:1], prev_energy)
    next_pos = jnp.where(at_end, end_positions[1:], next_pos)
    next_energy = jnp.where(at_end, end_energy[1:], next_energy)
    is_climb = climb_index == image_index
    neb_force = neb_project(
        force,
        positions,
        prev_pos,
        next_pos,
        energy,
        prev_energy,
        next_energy,
        tangent_kind,
        is_climb,
    )
    return (neb_force, energy)


def solution(mesh):
    in_specs = (
        P("image", "band", None, "ga"),
        P("image", "band"),
        P(None, None, "ga"),
        P(None, "ga"),
        P(),
        P(),
        P(),
        P("image", None, None),
        P("image"),
        P("image", None, None),
        P(),
        P(),
        P(),
        P("image"),
    )
    out_specs = (P("image", None, None), P("image"))
    return jax.shard_map(
        per_device, mesh=mesh, in_specs=in_specs, out_specs=out_specs, check_vma=False
    )
```

```python
import functools

import jax
import jax.numpy as jnp
from jax import lax
from jax.experimental import pallas as pl
from jax.experimental.pallas import tpu as pltpu
from jax.sharding import PartitionSpec as P

ATOMS = 64
PMAX = 8
SPECIES = 4


spring_constant = 5.0
BLOCKS = 16
CUTS = ((0, 4), (4, 4))


S2=(7.07106765e-01, -2.94627488e-02, 3.68265567e-04, -2.18770204e-06, 7.15483753e-09)
C2=(1.41421350e+00, -1.76776359e-01, 3.68257460e-03, -3.06124985e-05, 1.27899789e-07)
P1=6.283203125; P2=-1.781782029e-05; IT=0.15915494309189535

def cos_negsin(x):
    k = jnp.round(x*IT)
    r = (x - k*P1) - k*P2
    y = r*r
    s = S2[4]
    for q in S2[3::-1]: s = s*y + q
    s = s*r
    c = C2[4]
    for q in C2[3::-1]: c = c*y + q
    return 1.0 - s*s, -(s*c)

def make_chunk(waves, ff_ref, g_ref, pos_ref, live_ref, trig, stk, off):
    cs, sn, fm = trig
    chunk = stk.shape[1] // 2
    atoms = pos_ref.shape[1]
    for j in range(chunk // 128):
        here = pl.ds(off + 128 * j, 128)
        real = pl.ds(128 * j, 128)
        imag = pl.ds(chunk + 128 * j, 128)
        g = [g_ref[c : c + 1, here] for c in range(3)]
        for s in range(ff_ref.shape[0]):
            fm[j, s] = ff_ref[s, :, here] * live_ref[s]
        for a in range(0, atoms, 8):
            phase = pos_ref[0, a : a + 8, :] * g[0]
            phase = phase + pos_ref[1, a : a + 8, :] * g[1]
            phase = phase + pos_ref[2, a : a + 8, :] * g[2]
            cosine, neg_sine = cos_negsin(phase)
            cs[j, a : a + 8, :] = cosine
            sn[j, a : a + 8, :] = neg_sine
        row = 0
        for w_ref in waves:
            bands = w_ref.shape[0] // 2
            for n in range(0, bands, 16):
                u_in = w_ref[n : n + 16, here]
                v_in = w_ref[bands + n : bands + n + 16, here]
                stk[row + n : row + n + 16, real] = u_in.astype(jnp.bfloat16)
                stk[row + n : row + n + 16, imag] = v_in.astype(jnp.bfloat16)
                u = u_in.astype(jnp.float32)
                v = v_in.astype(jnp.float32)
                for c in range(3):
                    at = row + (c + 1) * bands + n
                    stk[at : at + 16, real] = (v * (-g[c])).astype(jnp.bfloat16)
                    stk[at : at + 16, imag] = (u * g[c]).astype(jnp.bfloat16)
            row += 4 * bands


def multiply_chunk(sp, acc, trig, stk, rb):
    cs, sn, fm = trig
    lanes, _, pmax, _ = fm.shape
    step = 16 // pmax
    for r0 in range(0, acc.shape[0], rb):
        rows = []
        for a in range(r0 // pmax, (r0 + rb) // pmax, step):
            parts = []
            for t in (cs, sn):
                for j in range(lanes):
                    terms = [
                        fm[j, sp[b]] * t[j, pl.ds(b, pmax, stride=0), :]
                        for b in range(a, a + step)
                    ]
                    parts.append(jnp.concatenate(terms, 0).astype(jnp.bfloat16))
            rows.append(jnp.concatenate(parts, 1))
        acc[r0 : r0 + rb, :] += lax.dot_general(
            jnp.concatenate(rows, 0),
            stk[...],
            (((1,), (1,)), ((), ())),
            preferred_element_type=jnp.float32,
        )


def contract_kernel(*refs, parts, gc, rb):
    sp, _, ff_ref, g_ref, pos_ref, live_ref = refs[:6]
    waves = refs[6 : 6 + parts]
    outs = refs[6 + parts : 6 + 2 * parts]
    acc, csa, sna, fma, csb, snb, fmb, stka, stkb = refs[6 + 2 * parts :]
    i = pl.program_id(0)
    first = (csa, sna, fma)
    second = (csb, snb, fmb)

    @pl.when(i == 0)
    def _():
        for ref in (acc, csb, snb, fmb, stkb):
            ref[...] = jnp.zeros_like(ref)

    def step(t, carry):
        base = pl.multiple_of(t * 2 * gc, 128)
        make_chunk(waves, ff_ref, g_ref, pos_ref, live_ref, first, stka, base)
        multiply_chunk(sp, acc, second, stkb, rb)
        make_chunk(waves, ff_ref, g_ref, pos_ref, live_ref, second, stkb, base + gc)
        multiply_chunk(sp, acc, first, stka, rb)
        return carry

    lax.fori_loop(0, g_ref.shape[1] // (2 * gc), step, 0)

    @pl.when(i == pl.num_programs(0) - 1)
    def _():
        multiply_chunk(sp, acc, second, stkb, rb)
        cols = outs[0].shape[1]
        for k in range(parts):
            outs[k][...] = 2.0 * acc[:, k * cols : (k + 1) * cols]


def contract(sp, start, waves, ff, g, posb, live, gc=1024, blk=4096, rb=256):
    nspec, pmax, _ = ff.shape
    atoms = posb.shape[1]
    parts = len(waves)
    length = waves[0].shape[1]
    rows, cols = atoms * pmax, 2 * waves[0].shape[0]
    trig = [
        pltpu.VMEM((gc // 128, atoms, 128), jnp.float32),
        pltpu.VMEM((gc // 128, atoms, 128), jnp.float32),
        pltpu.VMEM((gc // 128, nspec, pmax, 128), jnp.float32),
    ]
    stk = pltpu.VMEM((parts * cols, 2 * gc), jnp.bfloat16)
    return pl.pallas_call(
        functools.partial(contract_kernel, parts=parts, gc=gc, rb=rb),
        grid_spec=pltpu.PrefetchScalarGridSpec(
            num_scalar_prefetch=2,
            grid=(length // blk,),
            in_specs=[
                pl.BlockSpec((nspec, pmax, blk), lambda i, sp, st: (0, 0, st[0] + i)),
                pl.BlockSpec((3, blk), lambda i, sp, st: (0, st[0] + i)),
                pl.BlockSpec((3, atoms, 128), lambda i, sp, st: (0, 0, 0)),
                pl.BlockSpec((nspec, pmax, 128), lambda i, sp, st: (0, 0, 0)),
            ]
            + [pl.BlockSpec((w.shape[0], blk), lambda i, sp, st: (0, i)) for w in waves],
            out_specs=[pl.BlockSpec((rows, cols), lambda i, sp, st: (0, 0))] * parts,
            scratch_shapes=[pltpu.VMEM((rows, parts * cols), jnp.float32)]
            + trig * 2
            + [stk] * 2,
        ),
        out_shape=[jax.ShapeDtypeStruct((rows, cols), jnp.float32)] * parts,
        compiler_params=pltpu.CompilerParams(
            dimension_semantics=("arbitrary",), vmem_limit_bytes=48 * 2**20
        ),
        cost_estimate=pl.CostEstimate(
            flops=4 * rows * parts * cols * length,
            bytes_accessed=8 * length * (nspec * pmax + 3),
            transcendentals=0,
        ),
        name="contract",
    )(sp, start, ff, g, posb, live, *waves)


def passed_along(array, axis, by):
    length = lax.axis_size(axis)
    pairs = [(i, i + by) for i in range(length) if 0 <= i + by < length]
    return lax.ppermute(array, axis, pairs)


def atom_tables(species, proj_count, coupling):
    is_species = (species[:, None] == jnp.arange(SPECIES)[None, :]).astype(jnp.float32)
    is_live = (jnp.arange(PMAX)[None, :] < proj_count[:, None]).astype(jnp.float32)
    species_mask = is_species[:, :, None] * is_live[None, :, :]
    strength = jnp.sum(species_mask * coupling[None, :, :], axis=1)
    return (species_mask, strength)


def nonlocal_terms(proj_sums, occupied, strength):
    band_count = occupied.shape[0]
    atom_count = strength.shape[0]
    intersect = proj_sums[:, :band_count]
    weighted = intersect * occupied[None, :]
    energy_part = jnp.sum(strength.reshape(-1) * jnp.sum(weighted * intersect, axis=1))
    forces = []
    for axis_num in range(3):
        slope = proj_sums[:, (axis_num + 1) * band_count : (axis_num + 2) * band_count]
        per_row = jnp.sum(weighted * slope, axis=1).reshape(atom_count, PMAX)
        forces.append(-2.0 * jnp.sum(strength * per_row, axis=1))
    return (energy_part, jnp.stack(forces, axis=0))


def neb_project(
    force, here, prev_pos, next_pos, energy, prev_energy, next_energy, tangent_kind, is_climb
):
    to_next = next_pos - here
    from_prev = here - prev_pos
    rise_next = jnp.abs(next_energy - energy)
    rise_prev = jnp.abs(prev_energy - energy)
    larger = jnp.maximum(rise_next, rise_prev)
    smaller = jnp.minimum(rise_next, rise_prev)
    rising = next_energy > prev_energy
    weight_next = 1.0 + jnp.where(rising, larger, smaller)
    weight_prev = 1.0 + jnp.where(rising, smaller, larger)
    stiff_next = spring_constant * (1.0 + jax.nn.sigmoid(0.5 * (next_energy + energy)))
    stiff_prev = spring_constant * (1.0 + jax.nn.sigmoid(0.5 * (prev_energy + energy)))
    length_next = jnp.sqrt(jnp.sum(to_next * to_next, axis=(1, 2)) + 1.0)
    length_prev = jnp.sqrt(jnp.sum(from_prev * from_prev, axis=(1, 2)) + 1.0)
    upwind = weight_next[:, None, None] * to_next + weight_prev[:, None, None] * from_prev
    forward = to_next / length_next[:, None, None]
    backward = from_prev / length_prev[:, None, None]
    kind = tangent_kind[:, None, None]
    tangent = jnp.where(
        kind == 0,
        upwind,
        jnp.where(kind == 1, forward + backward, jnp.where(kind == 2, forward, backward)),
    )
    unit_tangent = tangent / jnp.sqrt(jnp.sum(tangent * tangent, axis=(1, 2)) + 1.0)[:, None, None]
    along = jnp.sum(force * unit_tangent, axis=(1, 2))[:, None, None]
    climbing = force - 2.0 * along * unit_tangent
    regular = (
        force
        - along * unit_tangent
        + (stiff_next * length_next - stiff_prev * length_prev)[:, None, None] * unit_tangent
    )
    return jnp.where(is_climb[:, None, None], climbing, regular)


def swapped(array, axis, mask):
    pairs = [(i, i ^ mask) for i in range(lax.axis_size(axis))]
    return lax.ppermute(array, axis, pairs)


def summed(array, axis):
    size = lax.axis_size(axis)
    if size & (size - 1):
        return lax.psum(array, axis)
    mask = 1
    while mask < size:
        array = array + swapped(array, axis, mask)
        mask *= 2
    return array


def scattered_rows(rows, axis):
    size = lax.axis_size(axis)
    index = lax.axis_index(axis)
    if size & (size - 1):
        block = rows.shape[0] // size
        return lax.psum_scatter(rows, axis, scatter_dimension=0, tiled=True), index * block
    first = jnp.int32(0)
    mask = 1
    while mask < size:
        half = rows.shape[0] // 2
        bit = (index // mask) % 2
        kept = lax.dynamic_slice_in_dim(rows, bit * half, half, 0)
        sent = lax.dynamic_slice_in_dim(rows, (1 - bit) * half, half, 0)
        rows = kept + swapped(sent, axis, mask)
        first = first + bit * half
        mask *= 2
    return rows, first


def per_device(
    wave_coeffs,
    occupation,
    form_factor,
    g_vectors,
    species,
    proj_count,
    coupling,
    positions,
    energy_rest,
    force_rest,
    end_positions,
    end_energy,
    climb_index,
    tangent_kind,
):
    species_mask, strength = atom_tables(species, proj_count, coupling)
    bands = wave_coeffs.shape[1]
    length = wave_coeffs.shape[3]
    is_live = (jnp.arange(PMAX)[None, :] < proj_count[:, None]).astype(jnp.float32)
    posb = jnp.broadcast_to(positions[0][:, :, None], (3, ATOMS, 128))
    live = jnp.broadcast_to(is_live[:, :, None], (SPECIES, PMAX, 128))
    blk = length // BLOCKS
    half = BLOCKS // 2
    core = lax.axis_index("band") % 2

    def rows_of(first, count):
        part = lax.dynamic_slice_in_dim(wave_coeffs[0], first * blk, count * blk, 2)
        return part.transpose(1, 0, 2).reshape(2 * bands, count * blk)

    chunks = []
    for at, count in CUTS:
        given = rows_of((1 - core) * half + at, count).astype(jnp.float32)
        chunks.append((core * half + at, count, swapped(given, "band", 1)))
    mine = 0.0
    other = 0.0
    for first, count, taken in chunks:
        kept = rows_of(first, count)
        start = first.astype(jnp.int32)[None]
        own_sums, other_sums = contract(
            species, start, [kept, taken], form_factor, g_vectors, posb, live, blk=blk
        )
        mine = mine + own_sums
        other = other + other_sums
    sums = mine + swapped(other, "band", 1)
    proj_sums, first_row = scattered_rows(sums, "ga")
    first_local = first_row // PMAX
    local_atoms = proj_sums.shape[0] // PMAX
    strength_part = lax.dynamic_slice_in_dim(strength, first_local, local_atoms, 0)
    energy_part, force_part = nonlocal_terms(proj_sums, occupation[0], strength_part)
    force_full = lax.dynamic_update_slice_in_dim(
        jnp.zeros((3, ATOMS), jnp.float32), force_part, first_local, 1
    )
    packed = jnp.concatenate(
        [force_full, jnp.full((1, ATOMS), energy_part, jnp.float32)], axis=0
    )
    packed = summed(summed(packed, "band"), "ga")
    energy = energy_rest + packed[3, :1]
    force = force_rest + packed[None, :3, :]
    image_index = lax.axis_index("image")
    image_count = lax.axis_size("image")
    sent = jnp.concatenate([positions[0], jnp.broadcast_to(energy[:, None], (1, ATOMS))], axis=0)
    before = passed_along(sent, "image", 1)
    after = passed_along(sent, "image", -1)
    prev_pos, prev_energy = before[None, :3, :], before[3, :1]
    next_pos, next_energy = after[None, :3, :], after[3, :1]
    at_start = image_index == 0
    at_end = image_index == image_count - 1
    prev_pos = jnp.where(at_start, end_positions[:1], prev_pos)
    prev_energy = jnp.where(at_start, end_energy[:1], prev_energy)
    next_pos = jnp.where(at_end, end_positions[1:], next_pos)
    next_energy = jnp.where(at_end, end_energy[1:], next_energy)
    is_climb = climb_index == image_index
    neb_force = neb_project(
        force,
        positions,
        prev_pos,
        next_pos,
        energy,
        prev_energy,
        next_energy,
        tangent_kind,
        is_climb,
    )
    return (neb_force, energy)


def solution(mesh):
    in_specs = (
        P("image", "band", None, "ga"),
        P("image", "band"),
        P(None, None, "ga"),
        P(None, "ga"),
        P(),
        P(),
        P(),
        P("image", None, None),
        P("image"),
        P("image", None, None),
        P(),
        P(),
        P(),
        P("image"),
    )
    out_specs = (P("image", None, None), P("image"))
    return jax.shard_map(
        per_device, mesh=mesh, in_specs=in_specs, out_specs=out_specs, check_vma=False
    )
```

```python
import functools

import jax
import jax.numpy as jnp
from jax import lax
from jax.experimental import pallas as pl
from jax.experimental.pallas import tpu as pltpu
from jax.sharding import PartitionSpec as P

ATOMS = 64
PMAX = 8
SPECIES = 4


spring_constant = 5.0
BLOCKS = 16
CUTS = ((0, 4), (4, 4))


S2=(7.07106765e-01, -2.94627488e-02, 3.68265567e-04, -2.18770204e-06, 7.15483753e-09)
C2=(1.41421350e+00, -1.76776359e-01, 3.68257460e-03, -3.06124985e-05, 1.27899789e-07)
P1=6.283203125; P2=-1.781782029e-05; IT=0.15915494309189535

def cos_negsin(x):
    k = jnp.round(x*IT)
    r = (x - k*P1) - k*P2
    y = r*r
    s = S2[4]
    for q in S2[3::-1]: s = s*y + q
    s = s*r
    c = C2[4]
    for q in C2[3::-1]: c = c*y + q
    return 1.0 - s*s, -(s*c)

def make_chunk(waves, ff_ref, g_ref, pos_ref, live_ref, trig, stk, off):
    cs, sn, fm = trig
    chunk = stk.shape[1] // 2
    atoms = pos_ref.shape[1]
    for j in range(chunk // 128):
        here = pl.ds(off + 128 * j, 128)
        real = pl.ds(128 * j, 128)
        imag = pl.ds(chunk + 128 * j, 128)
        g = [g_ref[c : c + 1, here] for c in range(3)]
        for s in range(ff_ref.shape[0]):
            fm[j, s] = ff_ref[s, :, here] * live_ref[s]
        for a in range(0, atoms, 8):
            phase = pos_ref[0, a : a + 8, :] * g[0]
            phase = phase + pos_ref[1, a : a + 8, :] * g[1]
            phase = phase + pos_ref[2, a : a + 8, :] * g[2]
            cosine, neg_sine = cos_negsin(phase)
            cs[j, a : a + 8, :] = cosine
            sn[j, a : a + 8, :] = neg_sine
        row = 0
        for w_ref in waves:
            bands = w_ref.shape[0] // 2
            for n in range(0, bands, 16):
                u_in = w_ref[n : n + 16, here]
                v_in = w_ref[bands + n : bands + n + 16, here]
                stk[row + n : row + n + 16, real] = u_in.astype(jnp.bfloat16)
                stk[row + n : row + n + 16, imag] = v_in.astype(jnp.bfloat16)
                u = u_in.astype(jnp.float32)
                v = v_in.astype(jnp.float32)
                for c in range(3):
                    at = row + (c + 1) * bands + n
                    stk[at : at + 16, real] = (v * (-g[c])).astype(jnp.bfloat16)
                    stk[at : at + 16, imag] = (u * g[c]).astype(jnp.bfloat16)
            row += 4 * bands


def multiply_chunk(sp, acc, trig, stk, rb):
    cs, sn, fm = trig
    lanes, _, pmax, _ = fm.shape
    step = 16 // pmax
    for r0 in range(0, acc.shape[0], rb):
        rows = []
        for a in range(r0 // pmax, (r0 + rb) // pmax, step):
            parts = []
            for t in (cs, sn):
                for j in range(lanes):
                    terms = [
                        fm[j, sp[b]] * t[j, pl.ds(b, pmax, stride=0), :]
                        for b in range(a, a + step)
                    ]
                    parts.append(jnp.concatenate(terms, 0).astype(jnp.bfloat16))
            rows.append(jnp.concatenate(parts, 1))
        acc[r0 : r0 + rb, :] += lax.dot_general(
            jnp.concatenate(rows, 0),
            stk[...],
            (((1,), (1,)), ((), ())),
            preferred_element_type=jnp.float32,
        )


def contract_kernel(*refs, parts, gc, rb):
    sp, _, ff_ref, g_ref, pos_ref, live_ref = refs[:6]
    waves = refs[6 : 6 + parts]
    outs = refs[6 + parts : 6 + 2 * parts]
    acc, csa, sna, fma, csb, snb, fmb, stka, stkb = refs[6 + 2 * parts :]
    i = pl.program_id(0)
    first = (csa, sna, fma)
    second = (csb, snb, fmb)

    @pl.when(i == 0)
    def _():
        for ref in (acc, csb, snb, fmb, stkb):
            ref[...] = jnp.zeros_like(ref)

    def step(t, carry):
        base = pl.multiple_of(t * 2 * gc, 128)
        make_chunk(waves, ff_ref, g_ref, pos_ref, live_ref, first, stka, base)
        multiply_chunk(sp, acc, second, stkb, rb)
        make_chunk(waves, ff_ref, g_ref, pos_ref, live_ref, second, stkb, base + gc)
        multiply_chunk(sp, acc, first, stka, rb)
        return carry

    lax.fori_loop(0, g_ref.shape[1] // (2 * gc), step, 0)

    @pl.when(i == pl.num_programs(0) - 1)
    def _():
        multiply_chunk(sp, acc, second, stkb, rb)
        cols = outs[0].shape[1]
        for k in range(parts):
            outs[k][...] = 2.0 * acc[:, k * cols : (k + 1) * cols]


def contract(sp, start, waves, ff, g, posb, live, gc=1024, blk=4096, rb=256):
    nspec, pmax, _ = ff.shape
    atoms = posb.shape[1]
    parts = len(waves)
    length = waves[0].shape[1]
    rows, cols = atoms * pmax, 2 * waves[0].shape[0]
    trig = [
        pltpu.VMEM((gc // 128, atoms, 128), jnp.float32),
        pltpu.VMEM((gc // 128, atoms, 128), jnp.float32),
        pltpu.VMEM((gc // 128, nspec, pmax, 128), jnp.float32),
    ]
    stk = pltpu.VMEM((parts * cols, 2 * gc), jnp.bfloat16)
    return pl.pallas_call(
        functools.partial(contract_kernel, parts=parts, gc=gc, rb=rb),
        grid_spec=pltpu.PrefetchScalarGridSpec(
            num_scalar_prefetch=2,
            grid=(length // blk,),
            in_specs=[
                pl.BlockSpec((nspec, pmax, blk), lambda i, sp, st: (0, 0, st[0] + i)),
                pl.BlockSpec((3, blk), lambda i, sp, st: (0, st[0] + i)),
                pl.BlockSpec((3, atoms, 128), lambda i, sp, st: (0, 0, 0)),
                pl.BlockSpec((nspec, pmax, 128), lambda i, sp, st: (0, 0, 0)),
            ]
            + [pl.BlockSpec((w.shape[0], blk), lambda i, sp, st: (0, i)) for w in waves],
            out_specs=[pl.BlockSpec((rows, cols), lambda i, sp, st: (0, 0))] * parts,
            scratch_shapes=[pltpu.VMEM((rows, parts * cols), jnp.float32)]
            + trig * 2
            + [stk] * 2,
        ),
        out_shape=[jax.ShapeDtypeStruct((rows, cols), jnp.float32)] * parts,
        compiler_params=pltpu.CompilerParams(
            dimension_semantics=("arbitrary",), vmem_limit_bytes=48 * 2**20
        ),
        cost_estimate=pl.CostEstimate(
            flops=4 * rows * parts * cols * length,
            bytes_accessed=8 * length * (nspec * pmax + 3),
            transcendentals=0,
        ),
        name="contract",
    )(sp, start, ff, g, posb, live, *waves)


def passed_along(array, axis, by):
    length = lax.axis_size(axis)
    pairs = [(i, i + by) for i in range(length) if 0 <= i + by < length]
    return lax.ppermute(array, axis, pairs)


def atom_tables(species, proj_count, coupling):
    is_species = (species[:, None] == jnp.arange(SPECIES)[None, :]).astype(jnp.float32)
    is_live = (jnp.arange(PMAX)[None, :] < proj_count[:, None]).astype(jnp.float32)
    species_mask = is_species[:, :, None] * is_live[None, :, :]
    strength = jnp.sum(species_mask * coupling[None, :, :], axis=1)
    return (species_mask, strength)


def total(array):
    return jnp.sum(array, axis=(0, 1), keepdims=True)


def terms_kernel(first_ref, sums_ref, occ_ref, strength_ref, out_ref):
    bands = occ_ref.shape[1]
    rows, atoms = sums_ref.shape[0], out_ref.shape[1]
    becp = sums_ref[:, :bands]
    weighted = becp * occ_ref[...]
    strength = strength_ref[...]
    row_atom = (first_ref[0] + lax.broadcasted_iota(jnp.int32, (rows, atoms), 0)) // PMAX
    mine = row_atom == lax.broadcasted_iota(jnp.int32, (rows, atoms), 1)
    for c in range(3):
        slope = sums_ref[:, (c + 1) * bands : (c + 2) * bands]
        per_row = strength * jnp.sum(weighted * slope, axis=1, keepdims=True)
        placed = jnp.where(mine, per_row, 0.0)
        out_ref[c : c + 1, :] = -2.0 * jnp.sum(placed, axis=0, keepdims=True)
    energy = total(strength * jnp.sum(weighted * becp, axis=1, keepdims=True))
    out_ref[3:4, :] = jnp.broadcast_to(energy, (1, atoms))


def nonlocal_terms(proj_sums, first_row, occupied, strength_rows):
    vmem = pl.BlockSpec(memory_space=pltpu.VMEM)
    return pl.pallas_call(
        terms_kernel,
        in_specs=[pl.BlockSpec(memory_space=pltpu.SMEM), vmem, vmem, vmem],
        out_specs=vmem,
        out_shape=jax.ShapeDtypeStruct((4, ATOMS), jnp.float32),
        name="terms",
    )(first_row[None], proj_sums, occupied, strength_rows)


def project_kernel(
    flags_ref, ends_ref, sent_ref, nl_ref, rest_ref, before_ref, after_ref, endpos_ref, out_ref
):
    at_start, at_end = flags_ref[0] == 1, flags_ref[1] == 1
    is_climb, kind = flags_ref[2] == 1, flags_ref[3]
    here = sent_ref[:3, :]
    energy = sent_ref[3:4, :1]
    force = rest_ref[...] + nl_ref[:3, :]
    prev_pos = jnp.where(at_start, endpos_ref[0], before_ref[:3, :])
    next_pos = jnp.where(at_end, endpos_ref[1], after_ref[:3, :])
    prev_energy = jnp.where(at_start, ends_ref[0], before_ref[3:4, :1])
    next_energy = jnp.where(at_end, ends_ref[1], after_ref[3:4, :1])
    to_next = next_pos - here
    from_prev = here - prev_pos
    rise_next = jnp.abs(next_energy - energy)
    rise_prev = jnp.abs(prev_energy - energy)
    larger = jnp.maximum(rise_next, rise_prev)
    smaller = jnp.minimum(rise_next, rise_prev)
    rising = next_energy > prev_energy
    weight_next = 1.0 + jnp.where(rising, larger, smaller)
    weight_prev = 1.0 + jnp.where(rising, smaller, larger)
    stiff_next = spring_constant * (1.0 + jax.nn.sigmoid(0.5 * (next_energy + energy)))
    stiff_prev = spring_constant * (1.0 + jax.nn.sigmoid(0.5 * (prev_energy + energy)))
    length_next = jnp.sqrt(total(to_next * to_next) + 1.0)
    length_prev = jnp.sqrt(total(from_prev * from_prev) + 1.0)
    upwind = weight_next * to_next + weight_prev * from_prev
    forward = to_next / length_next
    backward = from_prev / length_prev
    tangent = jnp.where(
        kind == 0,
        upwind,
        jnp.where(kind == 1, forward + backward, jnp.where(kind == 2, forward, backward)),
    )
    unit_tangent = tangent / jnp.sqrt(total(tangent * tangent) + 1.0)
    along = total(force * unit_tangent)
    spring = stiff_next * length_next - stiff_prev * length_prev
    scale = jnp.where(is_climb, -2.0 * along, spring - along)
    out_ref[...] = force + scale * unit_tangent


def neb_project(flags, end_energy, sent, packed, force_rest, before, after, end_positions):
    vmem = pl.BlockSpec(memory_space=pltpu.VMEM)
    smem = pl.BlockSpec(memory_space=pltpu.SMEM)
    return pl.pallas_call(
        project_kernel,
        in_specs=[smem, smem] + [vmem] * 6,
        out_specs=vmem,
        out_shape=jax.ShapeDtypeStruct((3, ATOMS), jnp.float32),
        name="project",
    )(flags, end_energy, sent, packed, force_rest, before, after, end_positions)


def swapped(array, axis, mask):
    pairs = [(i, i ^ mask) for i in range(lax.axis_size(axis))]
    return lax.ppermute(array, axis, pairs)


def summed(array, axis):
    size = lax.axis_size(axis)
    if size & (size - 1):
        return lax.psum(array, axis)
    mask = 1
    while mask < size:
        array = array + swapped(array, axis, mask)
        mask *= 2
    return array


def scattered_rows(rows, axis):
    size = lax.axis_size(axis)
    index = lax.axis_index(axis)
    if size & (size - 1):
        block = rows.shape[0] // size
        return lax.psum_scatter(rows, axis, scatter_dimension=0, tiled=True), index * block
    first = jnp.int32(0)
    mask = 1
    while mask < size:
        half = rows.shape[0] // 2
        bit = (index // mask) % 2
        kept = lax.dynamic_slice_in_dim(rows, bit * half, half, 0)
        sent = lax.dynamic_slice_in_dim(rows, (1 - bit) * half, half, 0)
        rows = kept + swapped(sent, axis, mask)
        first = first + (bit * half).astype(jnp.int32)
        mask *= 2
    return rows, first


def per_device(
    wave_coeffs,
    occupation,
    form_factor,
    g_vectors,
    species,
    proj_count,
    coupling,
    positions,
    energy_rest,
    force_rest,
    end_positions,
    end_energy,
    climb_index,
    tangent_kind,
):
    species_mask, strength = atom_tables(species, proj_count, coupling)
    bands = wave_coeffs.shape[1]
    length = wave_coeffs.shape[3]
    is_live = (jnp.arange(PMAX)[None, :] < proj_count[:, None]).astype(jnp.float32)
    posb = jnp.broadcast_to(positions[0][:, :, None], (3, ATOMS, 128))
    live = jnp.broadcast_to(is_live[:, :, None], (SPECIES, PMAX, 128))
    blk = length // BLOCKS
    half = BLOCKS // 2
    core = lax.axis_index("band") % 2

    def rows_of(first, count):
        part = lax.dynamic_slice_in_dim(wave_coeffs[0], first * blk, count * blk, 2)
        return part.transpose(1, 0, 2).reshape(2 * bands, count * blk)

    chunks = []
    for at, count in CUTS:
        given = rows_of((1 - core) * half + at, count).astype(jnp.float32)
        chunks.append((core * half + at, count, swapped(given, "band", 1)))
    mine = 0.0
    other = 0.0
    for first, count, taken in chunks:
        kept = rows_of(first, count)
        start = first.astype(jnp.int32)[None]
        own_sums, other_sums = contract(
            species, start, [kept, taken], form_factor, g_vectors, posb, live, blk=blk
        )
        mine = mine + own_sums
        other = other + other_sums
    sums = mine + swapped(other, "band", 1)
    proj_sums, first_row = scattered_rows(sums, "ga")
    strength_rows = lax.dynamic_slice_in_dim(
        strength.reshape(ATOMS * PMAX, 1), first_row, proj_sums.shape[0], 0
    )
    packed = nonlocal_terms(proj_sums, first_row, occupation, strength_rows)
    packed = summed(summed(packed, "band"), "ga")
    padded = jnp.concatenate([positions[0], jnp.zeros((1, ATOMS), jnp.float32)], axis=0)
    is_last = lax.broadcasted_iota(jnp.int32, padded.shape, 0) == 3
    sent = jnp.where(is_last, packed + energy_rest, padded)
    before = passed_along(sent, "image", 1)
    after = passed_along(sent, "image", -1)
    image_index = lax.axis_index("image")
    flags = jnp.stack(
        [
            (image_index == 0).astype(jnp.int32),
            (image_index == lax.axis_size("image") - 1).astype(jnp.int32),
            (climb_index[0] == image_index).astype(jnp.int32),
            tangent_kind[0],
        ]
    )
    neb_force = neb_project(
        flags, end_energy, sent, packed, force_rest[0], before, after, end_positions
    )
    return (neb_force[None], sent[3, :1])


def solution(mesh):
    in_specs = (
        P("image", "band", None, "ga"),
        P("image", "band"),
        P(None, None, "ga"),
        P(None, "ga"),
        P(),
        P(),
        P(),
        P("image", None, None),
        P("image"),
        P("image", None, None),
        P(),
        P(),
        P(),
        P("image"),
    )
    out_specs = (P("image", None, None), P("image"))
    return jax.shard_map(
        per_device, mesh=mesh, in_specs=in_specs, out_specs=out_specs, check_vma=False
    )
```

```python
import functools

import jax
import jax.numpy as jnp
from jax import lax
from jax.experimental import pallas as pl
from jax.experimental.pallas import tpu as pltpu
from jax.sharding import PartitionSpec as P

ATOMS = 64
PMAX = 8
SPECIES = 4


spring_constant = 5.0
BLOCKS = 16
CUTS = ((0, 4), (4, 4))


S2=(7.07106765e-01, -2.94627488e-02, 3.68265567e-04, -2.18770204e-06, 7.15483753e-09)
C2=(1.41421350e+00, -1.76776359e-01, 3.68257460e-03, -3.06124985e-05, 1.27899789e-07)
P1=6.283203125; P2=-1.781782029e-05; IT=0.15915494309189535

def cos_negsin(x):
    k = jnp.round(x*IT)
    r = (x - k*P1) - k*P2
    y = r*r
    s = S2[4]
    for q in S2[3::-1]: s = s*y + q
    s = s*r
    c = C2[4]
    for q in C2[3::-1]: c = c*y + q
    return 1.0 - s*s, -(s*c)

def make_chunk(waves, ff_ref, g_ref, pos_ref, live_ref, trig, stk, off):
    cs, sn, fm = trig
    chunk = stk.shape[1] // 2
    atoms = pos_ref.shape[1]
    for j in range(chunk // 128):
        here = pl.ds(off + 128 * j, 128)
        real = pl.ds(128 * j, 128)
        imag = pl.ds(chunk + 128 * j, 128)
        g = [g_ref[c : c + 1, here] for c in range(3)]
        for s in range(ff_ref.shape[0]):
            fm[j, s] = ff_ref[s, :, here] * live_ref[s]
        for a in range(0, atoms, 8):
            phase = pos_ref[0, a : a + 8, :] * g[0]
            phase = phase + pos_ref[1, a : a + 8, :] * g[1]
            phase = phase + pos_ref[2, a : a + 8, :] * g[2]
            cosine, neg_sine = cos_negsin(phase)
            cs[j, a : a + 8, :] = cosine
            sn[j, a : a + 8, :] = neg_sine
        row = 0
        for w_ref in waves:
            bands = w_ref.shape[0] // 2
            for n in range(0, bands, 16):
                u_in = w_ref[n : n + 16, here]
                v_in = w_ref[bands + n : bands + n + 16, here]
                stk[row + n : row + n + 16, real] = u_in.astype(jnp.bfloat16)
                stk[row + n : row + n + 16, imag] = v_in.astype(jnp.bfloat16)
                u = u_in.astype(jnp.float32)
                v = v_in.astype(jnp.float32)
                for c in range(3):
                    at = row + (c + 1) * bands + n
                    stk[at : at + 16, real] = (v * (-g[c])).astype(jnp.bfloat16)
                    stk[at : at + 16, imag] = (u * g[c]).astype(jnp.bfloat16)
            row += 4 * bands


def multiply_chunk(sp, acc, trig, stk, rb):
    cs, sn, fm = trig
    lanes, _, pmax, _ = fm.shape
    step = 16 // pmax
    for r0 in range(0, acc.shape[0], rb):
        rows = []
        for a in range(r0 // pmax, (r0 + rb) // pmax, step):
            parts = []
            for t in (cs, sn):
                for j in range(lanes):
                    terms = [
                        fm[j, sp[b]] * t[j, pl.ds(b, pmax, stride=0), :]
                        for b in range(a, a + step)
                    ]
                    parts.append(jnp.concatenate(terms, 0).astype(jnp.bfloat16))
            rows.append(jnp.concatenate(parts, 1))
        acc[r0 : r0 + rb, :] += lax.dot_general(
            jnp.concatenate(rows, 0),
            stk[...],
            (((1,), (1,)), ((), ())),
            preferred_element_type=jnp.float32,
        )


def contract_kernel(*refs, parts, gc, rb):
    sp, _, ff_ref, g_ref, pos_ref, live_ref = refs[:6]
    waves = refs[6 : 6 + parts]
    outs = refs[6 + parts : 6 + 2 * parts]
    acc, csa, sna, fma, csb, snb, fmb, stka, stkb = refs[6 + 2 * parts :]
    i = pl.program_id(0)
    first = (csa, sna, fma)
    second = (csb, snb, fmb)

    @pl.when(i == 0)
    def _():
        for ref in (acc, csb, snb, fmb, stkb):
            ref[...] = jnp.zeros_like(ref)

    def step(t, carry):
        base = pl.multiple_of(t * 2 * gc, 128)
        make_chunk(waves, ff_ref, g_ref, pos_ref, live_ref, first, stka, base)
        multiply_chunk(sp, acc, second, stkb, rb)
        make_chunk(waves, ff_ref, g_ref, pos_ref, live_ref, second, stkb, base + gc)
        multiply_chunk(sp, acc, first, stka, rb)
        return carry

    lax.fori_loop(0, g_ref.shape[1] // (2 * gc), step, 0)

    @pl.when(i == pl.num_programs(0) - 1)
    def _():
        multiply_chunk(sp, acc, second, stkb, rb)
        cols = outs[0].shape[1]
        for k in range(parts):
            outs[k][...] = 2.0 * acc[:, k * cols : (k + 1) * cols]


def contract(sp, start, waves, ff, g, posb, live, gc=1024, blk=4096, rb=256):
    nspec, pmax, _ = ff.shape
    atoms = posb.shape[1]
    parts = len(waves)
    length = waves[0].shape[1]
    rows, cols = atoms * pmax, 2 * waves[0].shape[0]
    trig = [
        pltpu.VMEM((gc // 128, atoms, 128), jnp.float32),
        pltpu.VMEM((gc // 128, atoms, 128), jnp.float32),
        pltpu.VMEM((gc // 128, nspec, pmax, 128), jnp.float32),
    ]
    stk = pltpu.VMEM((parts * cols, 2 * gc), jnp.bfloat16)
    return pl.pallas_call(
        functools.partial(contract_kernel, parts=parts, gc=gc, rb=rb),
        grid_spec=pltpu.PrefetchScalarGridSpec(
            num_scalar_prefetch=2,
            grid=(length // blk,),
            in_specs=[
                pl.BlockSpec((nspec, pmax, blk), lambda i, sp, st: (0, 0, st[0] + i)),
                pl.BlockSpec((3, blk), lambda i, sp, st: (0, st[0] + i)),
                pl.BlockSpec((3, atoms, 128), lambda i, sp, st: (0, 0, 0)),
                pl.BlockSpec((nspec, pmax, 128), lambda i, sp, st: (0, 0, 0)),
            ]
            + [pl.BlockSpec((w.shape[0], blk), lambda i, sp, st: (0, i)) for w in waves],
            out_specs=[pl.BlockSpec((rows, cols), lambda i, sp, st: (0, 0))] * parts,
            scratch_shapes=[pltpu.VMEM((rows, parts * cols), jnp.float32)]
            + trig * 2
            + [stk] * 2,
        ),
        out_shape=[jax.ShapeDtypeStruct((rows, cols), jnp.float32)] * parts,
        compiler_params=pltpu.CompilerParams(
            dimension_semantics=("arbitrary",), vmem_limit_bytes=48 * 2**20
        ),
        cost_estimate=pl.CostEstimate(
            flops=4 * rows * parts * cols * length,
            bytes_accessed=8 * length * (nspec * pmax + 3),
            transcendentals=0,
        ),
        name="contract",
    )(sp, start, ff, g, posb, live, *waves)


def passed_along(array, axis, by):
    length = lax.axis_size(axis)
    pairs = [(i, i + by) for i in range(length) if 0 <= i + by < length]
    return lax.ppermute(array, axis, pairs)


def atom_tables(species, proj_count, coupling):
    is_species = (species[:, None] == jnp.arange(SPECIES)[None, :]).astype(jnp.float32)
    is_live = (jnp.arange(PMAX)[None, :] < proj_count[:, None]).astype(jnp.float32)
    species_mask = is_species[:, :, None] * is_live[None, :, :]
    strength = jnp.sum(species_mask * coupling[None, :, :], axis=1)
    return (species_mask, strength)


def total(array):
    return jnp.sum(array, axis=(0, 1), keepdims=True)


def terms_kernel(first_ref, sums_ref, occ_ref, strength_ref, out_ref):
    bands = occ_ref.shape[1]
    rows, atoms = sums_ref.shape[0], out_ref.shape[1]
    becp = sums_ref[:, :bands]
    weighted = becp * occ_ref[...]
    strength = strength_ref[...]
    row_atom = (first_ref[0] + lax.broadcasted_iota(jnp.int32, (rows, atoms), 0)) // PMAX
    mine = row_atom == lax.broadcasted_iota(jnp.int32, (rows, atoms), 1)
    for c in range(3):
        slope = sums_ref[:, (c + 1) * bands : (c + 2) * bands]
        per_row = strength * jnp.sum(weighted * slope, axis=1, keepdims=True)
        placed = jnp.where(mine, per_row, 0.0)
        out_ref[c : c + 1, :] = -2.0 * jnp.sum(placed, axis=0, keepdims=True)
    energy = total(strength * jnp.sum(weighted * becp, axis=1, keepdims=True))
    out_ref[3:4, :] = jnp.broadcast_to(energy, (1, atoms))


def nonlocal_terms(proj_sums, first_row, occupied, strength_rows):
    vmem = pl.BlockSpec(memory_space=pltpu.VMEM)
    return pl.pallas_call(
        terms_kernel,
        in_specs=[pl.BlockSpec(memory_space=pltpu.SMEM), vmem, vmem, vmem],
        out_specs=vmem,
        out_shape=jax.ShapeDtypeStruct((4, ATOMS), jnp.float32),
        name="terms",
    )(first_row[None], proj_sums, occupied, strength_rows)


def project_kernel(
    flags_ref, ends_ref, sent_ref, nl_ref, rest_ref, before_ref, after_ref, endpos_ref, out_ref
):
    at_start, at_end = flags_ref[0] == 1, flags_ref[1] == 1
    is_climb, kind = flags_ref[2] == 1, flags_ref[3]
    here = sent_ref[:3, :]
    energy = sent_ref[3:4, :1]
    force = rest_ref[...] + nl_ref[:3, :]
    prev_pos = jnp.where(at_start, endpos_ref[0], before_ref[:3, :])
    next_pos = jnp.where(at_end, endpos_ref[1], after_ref[:3, :])
    prev_energy = jnp.where(at_start, ends_ref[0], before_ref[3:4, :1])
    next_energy = jnp.where(at_end, ends_ref[1], after_ref[3:4, :1])
    to_next = next_pos - here
    from_prev = here - prev_pos
    rise_next = jnp.abs(next_energy - energy)
    rise_prev = jnp.abs(prev_energy - energy)
    larger = jnp.maximum(rise_next, rise_prev)
    smaller = jnp.minimum(rise_next, rise_prev)
    rising = next_energy > prev_energy
    weight_next = 1.0 + jnp.where(rising, larger, smaller)
    weight_prev = 1.0 + jnp.where(rising, smaller, larger)
    stiff_next = spring_constant * (1.0 + jax.nn.sigmoid(0.5 * (next_energy + energy)))
    stiff_prev = spring_constant * (1.0 + jax.nn.sigmoid(0.5 * (prev_energy + energy)))
    length_next = jnp.sqrt(total(to_next * to_next) + 1.0)
    length_prev = jnp.sqrt(total(from_prev * from_prev) + 1.0)
    upwind = weight_next * to_next + weight_prev * from_prev
    forward = to_next / length_next
    backward = from_prev / length_prev
    tangent = jnp.where(
        kind == 0,
        upwind,
        jnp.where(kind == 1, forward + backward, jnp.where(kind == 2, forward, backward)),
    )
    unit_tangent = tangent / jnp.sqrt(total(tangent * tangent) + 1.0)
    along = total(force * unit_tangent)
    spring = stiff_next * length_next - stiff_prev * length_prev
    scale = jnp.where(is_climb, -2.0 * along, spring - along)
    out_ref[:, 0, :] = force + scale * unit_tangent


def neb_project(flags, end_energy, sent, packed, force_rest, before, after, end_positions):
    vmem = pl.BlockSpec(memory_space=pltpu.VMEM)
    smem = pl.BlockSpec(memory_space=pltpu.SMEM)
    return pl.pallas_call(
        project_kernel,
        in_specs=[smem, smem] + [vmem] * 6,
        out_specs=vmem,
        out_shape=jax.ShapeDtypeStruct((3, 1, ATOMS), jnp.float32),
        name="project",
    )(flags, end_energy, sent, packed, force_rest, before, after, end_positions)


def swapped(array, axis, mask):
    pairs = [(i, i ^ mask) for i in range(lax.axis_size(axis))]
    return lax.ppermute(array, axis, pairs)


def summed(array, axis):
    size = lax.axis_size(axis)
    if size & (size - 1):
        return lax.psum(array, axis)
    mask = 1
    while mask < size:
        array = array + swapped(array, axis, mask)
        mask *= 2
    return array


def scattered_rows(rows, axis):
    size = lax.axis_size(axis)
    index = lax.axis_index(axis)
    if size & (size - 1):
        block = rows.shape[0] // size
        return lax.psum_scatter(rows, axis, scatter_dimension=0, tiled=True), index * block
    first = jnp.int32(0)
    mask = 1
    while mask < size:
        half = rows.shape[0] // 2
        bit = (index // mask) % 2
        kept = lax.dynamic_slice_in_dim(rows, bit * half, half, 0)
        sent = lax.dynamic_slice_in_dim(rows, (1 - bit) * half, half, 0)
        rows = kept + swapped(sent, axis, mask)
        first = first + (bit * half).astype(jnp.int32)
        mask *= 2
    return rows, first


def per_device(
    wave_coeffs,
    occupation,
    form_factor,
    g_vectors,
    species,
    proj_count,
    coupling,
    positions,
    energy_rest,
    force_rest,
    end_positions,
    end_energy,
    climb_index,
    tangent_kind,
):
    species_mask, strength = atom_tables(species, proj_count, coupling)
    bands = wave_coeffs.shape[1]
    length = wave_coeffs.shape[3]
    is_live = (jnp.arange(PMAX)[None, :] < proj_count[:, None]).astype(jnp.float32)
    posb = jnp.broadcast_to(positions[0][:, :, None], (3, ATOMS, 128))
    live = jnp.broadcast_to(is_live[:, :, None], (SPECIES, PMAX, 128))
    blk = length // BLOCKS
    half = BLOCKS // 2
    core = lax.axis_index("band") % 2

    def rows_of(first, count):
        part = lax.dynamic_slice_in_dim(wave_coeffs[0], first * blk, count * blk, 2)
        return part.transpose(1, 0, 2).reshape(2 * bands, count * blk)

    chunks = []
    for at, count in CUTS:
        given = rows_of((1 - core) * half + at, count).astype(jnp.float32)
        chunks.append((core * half + at, count, swapped(given, "band", 1)))
    mine = 0.0
    other = 0.0
    for first, count, taken in chunks:
        kept = rows_of(first, count)
        start = first.astype(jnp.int32)[None]
        own_sums, other_sums = contract(
            species, start, [kept, taken], form_factor, g_vectors, posb, live, blk=blk
        )
        mine = mine + own_sums
        other = other + other_sums
    sums = mine + swapped(other, "band", 1)
    proj_sums, first_row = scattered_rows(sums, "ga")
    strength_rows = lax.dynamic_slice_in_dim(
        strength.reshape(ATOMS * PMAX, 1), first_row, proj_sums.shape[0], 0
    )
    packed = nonlocal_terms(proj_sums, first_row, occupation, strength_rows)
    packed = summed(summed(packed, "band"), "ga")
    padded = jnp.concatenate([positions[0], jnp.zeros((1, ATOMS), jnp.float32)], axis=0)
    is_last = lax.broadcasted_iota(jnp.int32, padded.shape, 0) == 3
    sent = jnp.where(is_last, packed + energy_rest, padded)
    before = passed_along(sent, "image", 1)
    after = passed_along(sent, "image", -1)
    image_index = lax.axis_index("image")
    flags = jnp.stack(
        [
            (image_index == 0).astype(jnp.int32),
            (image_index == lax.axis_size("image") - 1).astype(jnp.int32),
            (climb_index[0] == image_index).astype(jnp.int32),
            tangent_kind[0],
        ]
    )
    neb_force = neb_project(
        flags, end_energy, sent, packed, force_rest[0], before, after, end_positions
    )
    return (neb_force.transpose(1, 0, 2), sent[3, :1])


def solution(mesh):
    in_specs = (
        P("image", "band", None, "ga"),
        P("image", "band"),
        P(None, None, "ga"),
        P(None, "ga"),
        P(),
        P(),
        P(),
        P("image", None, None),
        P("image"),
        P("image", None, None),
        P(),
        P(),
        P(),
        P("image"),
    )
    out_specs = (P("image", None, None), P("image"))
    return jax.shard_map(
        per_device, mesh=mesh, in_specs=in_specs, out_specs=out_specs, check_vma=False
    )
```

```python
import functools

import jax
import jax.numpy as jnp
from jax import lax
from jax.experimental import pallas as pl
from jax.experimental.pallas import tpu as pltpu
from jax.sharding import PartitionSpec as P

ATOMS = 64
PMAX = 8
SPECIES = 4


spring_constant = 5.0
BLOCKS = 16
CUTS = ((0, 4), (4, 4))


S2=(7.07106765e-01, -2.94627488e-02, 3.68265567e-04, -2.18770204e-06, 7.15483753e-09)
C2=(1.41421350e+00, -1.76776359e-01, 3.68257460e-03, -3.06124985e-05, 1.27899789e-07)
P1=6.283203125; P2=-1.781782029e-05; IT=0.15915494309189535

def cos_negsin(x):
    k = jnp.round(x*IT)
    r = (x - k*P1) - k*P2
    y = r*r
    s = S2[4]
    for q in S2[3::-1]: s = s*y + q
    s = s*r
    c = C2[4]
    for q in C2[3::-1]: c = c*y + q
    return 1.0 - s*s, -(s*c)

def make_chunk(waves, ff_ref, g_ref, pos_ref, live_ref, trig, stk, off):
    cs, sn, fm = trig
    chunk = stk.shape[1] // 2
    atoms = pos_ref.shape[1]
    for j in range(chunk // 128):
        here = pl.ds(off + 128 * j, 128)
        real = pl.ds(128 * j, 128)
        imag = pl.ds(chunk + 128 * j, 128)
        g = [g_ref[c : c + 1, here] for c in range(3)]
        for s in range(ff_ref.shape[0]):
            fm[j, s] = ff_ref[s, :, here] * live_ref[s]
        for a in range(0, atoms, 8):
            phase = pos_ref[0, a : a + 8, :] * g[0]
            phase = phase + pos_ref[1, a : a + 8, :] * g[1]
            phase = phase + pos_ref[2, a : a + 8, :] * g[2]
            cosine, neg_sine = cos_negsin(phase)
            cs[j, a : a + 8, :] = cosine
            sn[j, a : a + 8, :] = neg_sine
        row = 0
        for w_ref in waves:
            bands = w_ref.shape[0] // 2
            for n in range(0, bands, 16):
                u_in = w_ref[n : n + 16, here]
                v_in = w_ref[bands + n : bands + n + 16, here]
                stk[row + n : row + n + 16, real] = u_in.astype(jnp.bfloat16)
                stk[row + n : row + n + 16, imag] = v_in.astype(jnp.bfloat16)
                u = u_in.astype(jnp.float32)
                v = v_in.astype(jnp.float32)
                for c in range(3):
                    at = row + (c + 1) * bands + n
                    stk[at : at + 16, real] = (v * (-g[c])).astype(jnp.bfloat16)
                    stk[at : at + 16, imag] = (u * g[c]).astype(jnp.bfloat16)
            row += 4 * bands


def multiply_chunk(sp, acc, trig, stk, rb):
    cs, sn, fm = trig
    lanes, _, pmax, _ = fm.shape
    step = 16 // pmax
    for r0 in range(0, acc.shape[0], rb):
        rows = []
        for a in range(r0 // pmax, (r0 + rb) // pmax, step):
            parts = []
            for t in (cs, sn):
                for j in range(lanes):
                    terms = [
                        fm[j, sp[b]] * t[j, pl.ds(b, pmax, stride=0), :]
                        for b in range(a, a + step)
                    ]
                    parts.append(jnp.concatenate(terms, 0).astype(jnp.bfloat16))
            rows.append(jnp.concatenate(parts, 1))
        acc[r0 : r0 + rb, :] += lax.dot_general(
            jnp.concatenate(rows, 0),
            stk[...],
            (((1,), (1,)), ((), ())),
            preferred_element_type=jnp.float32,
        )


def contract_kernel(*refs, parts, gc, rb):
    sp, _, ff_ref, g_ref, pos_ref, live_ref = refs[:6]
    waves = refs[6 : 6 + parts]
    outs = refs[6 + parts : 6 + 2 * parts]
    acc, csa, sna, fma, csb, snb, fmb, stka, stkb = refs[6 + 2 * parts :]
    i = pl.program_id(0)
    first = (csa, sna, fma)
    second = (csb, snb, fmb)

    @pl.when(i == 0)
    def _():
        for ref in (acc, csb, snb, fmb, stkb):
            ref[...] = jnp.zeros_like(ref)

    def step(t, carry):
        base = pl.multiple_of(t * 2 * gc, 128)
        make_chunk(waves, ff_ref, g_ref, pos_ref, live_ref, first, stka, base)
        multiply_chunk(sp, acc, second, stkb, rb)
        make_chunk(waves, ff_ref, g_ref, pos_ref, live_ref, second, stkb, base + gc)
        multiply_chunk(sp, acc, first, stka, rb)
        return carry

    lax.fori_loop(0, g_ref.shape[1] // (2 * gc), step, 0)

    @pl.when(i == pl.num_programs(0) - 1)
    def _():
        multiply_chunk(sp, acc, second, stkb, rb)
        cols = outs[0].shape[1]
        for k in range(parts):
            outs[k][...] = 2.0 * acc[:, k * cols : (k + 1) * cols]


def contract(sp, start, waves, ff, g, posb, live, gc=2048, blk=4096, rb=256):
    gc = min(gc, blk // 2)
    nspec, pmax, _ = ff.shape
    atoms = posb.shape[1]
    parts = len(waves)
    length = waves[0].shape[1]
    rows, cols = atoms * pmax, 2 * waves[0].shape[0]
    trig = [
        pltpu.VMEM((gc // 128, atoms, 128), jnp.float32),
        pltpu.VMEM((gc // 128, atoms, 128), jnp.float32),
        pltpu.VMEM((gc // 128, nspec, pmax, 128), jnp.float32),
    ]
    stk = pltpu.VMEM((parts * cols, 2 * gc), jnp.bfloat16)
    return pl.pallas_call(
        functools.partial(contract_kernel, parts=parts, gc=gc, rb=rb),
        grid_spec=pltpu.PrefetchScalarGridSpec(
            num_scalar_prefetch=2,
            grid=(length // blk,),
            in_specs=[
                pl.BlockSpec((nspec, pmax, blk), lambda i, sp, st: (0, 0, st[0] + i)),
                pl.BlockSpec((3, blk), lambda i, sp, st: (0, st[0] + i)),
                pl.BlockSpec((3, atoms, 128), lambda i, sp, st: (0, 0, 0)),
                pl.BlockSpec((nspec, pmax, 128), lambda i, sp, st: (0, 0, 0)),
            ]
            + [pl.BlockSpec((w.shape[0], blk), lambda i, sp, st: (0, i)) for w in waves],
            out_specs=[pl.BlockSpec((rows, cols), lambda i, sp, st: (0, 0))] * parts,
            scratch_shapes=[pltpu.VMEM((rows, parts * cols), jnp.float32)]
            + trig * 2
            + [stk] * 2,
        ),
        out_shape=[jax.ShapeDtypeStruct((rows, cols), jnp.float32)] * parts,
        compiler_params=pltpu.CompilerParams(
            dimension_semantics=("arbitrary",), vmem_limit_bytes=48 * 2**20
        ),
        cost_estimate=pl.CostEstimate(
            flops=4 * rows * parts * cols * length,
            bytes_accessed=8 * length * (nspec * pmax + 3),
            transcendentals=0,
        ),
        name="contract",
    )(sp, start, ff, g, posb, live, *waves)


def passed_along(array, axis, by):
    length = lax.axis_size(axis)
    pairs = [(i, i + by) for i in range(length) if 0 <= i + by < length]
    return lax.ppermute(array, axis, pairs)


def atom_tables(species, proj_count, coupling):
    is_species = (species[:, None] == jnp.arange(SPECIES)[None, :]).astype(jnp.float32)
    is_live = (jnp.arange(PMAX)[None, :] < proj_count[:, None]).astype(jnp.float32)
    species_mask = is_species[:, :, None] * is_live[None, :, :]
    strength = jnp.sum(species_mask * coupling[None, :, :], axis=1)
    return (species_mask, strength)


def total(array):
    return jnp.sum(array, axis=(0, 1), keepdims=True)


def terms_kernel(first_ref, sums_ref, occ_ref, strength_ref, out_ref):
    bands = occ_ref.shape[1]
    rows, atoms = sums_ref.shape[0], out_ref.shape[1]
    becp = sums_ref[:, :bands]
    weighted = becp * occ_ref[...]
    strength = strength_ref[...]
    row_atom = (first_ref[0] + lax.broadcasted_iota(jnp.int32, (rows, atoms), 0)) // PMAX
    mine = row_atom == lax.broadcasted_iota(jnp.int32, (rows, atoms), 1)
    for c in range(3):
        slope = sums_ref[:, (c + 1) * bands : (c + 2) * bands]
        per_row = strength * jnp.sum(weighted * slope, axis=1, keepdims=True)
        placed = jnp.where(mine, per_row, 0.0)
        out_ref[c : c + 1, :] = -2.0 * jnp.sum(placed, axis=0, keepdims=True)
    energy = total(strength * jnp.sum(weighted * becp, axis=1, keepdims=True))
    out_ref[3:4, :] = jnp.broadcast_to(energy, (1, atoms))


def nonlocal_terms(proj_sums, first_row, occupied, strength_rows):
    vmem = pl.BlockSpec(memory_space=pltpu.VMEM)
    return pl.pallas_call(
        terms_kernel,
        in_specs=[pl.BlockSpec(memory_space=pltpu.SMEM), vmem, vmem, vmem],
        out_specs=vmem,
        out_shape=jax.ShapeDtypeStruct((4, ATOMS), jnp.float32),
        name="terms",
    )(first_row[None], proj_sums, occupied, strength_rows)


def project_kernel(
    flags_ref, ends_ref, sent_ref, nl_ref, rest_ref, before_ref, after_ref, endpos_ref, out_ref
):
    at_start, at_end = flags_ref[0] == 1, flags_ref[1] == 1
    is_climb, kind = flags_ref[2] == 1, flags_ref[3]
    here = sent_ref[:3, :]
    energy = sent_ref[3:4, :1]
    force = rest_ref[...] + nl_ref[:3, :]
    prev_pos = jnp.where(at_start, endpos_ref[0], before_ref[:3, :])
    next_pos = jnp.where(at_end, endpos_ref[1], after_ref[:3, :])
    prev_energy = jnp.where(at_start, ends_ref[0], before_ref[3:4, :1])
    next_energy = jnp.where(at_end, ends_ref[1], after_ref[3:4, :1])
    to_next = next_pos - here
    from_prev = here - prev_pos
    rise_next = jnp.abs(next_energy - energy)
    rise_prev = jnp.abs(prev_energy - energy)
    larger = jnp.maximum(rise_next, rise_prev)
    smaller = jnp.minimum(rise_next, rise_prev)
    rising = next_energy > prev_energy
    weight_next = 1.0 + jnp.where(rising, larger, smaller)
    weight_prev = 1.0 + jnp.where(rising, smaller, larger)
    stiff_next = spring_constant * (1.0 + jax.nn.sigmoid(0.5 * (next_energy + energy)))
    stiff_prev = spring_constant * (1.0 + jax.nn.sigmoid(0.5 * (prev_energy + energy)))
    length_next = jnp.sqrt(total(to_next * to_next) + 1.0)
    length_prev = jnp.sqrt(total(from_prev * from_prev) + 1.0)
    upwind = weight_next * to_next + weight_prev * from_prev
    forward = to_next / length_next
    backward = from_prev / length_prev
    tangent = jnp.where(
        kind == 0,
        upwind,
        jnp.where(kind == 1, forward + backward, jnp.where(kind == 2, forward, backward)),
    )
    unit_tangent = tangent / jnp.sqrt(total(tangent * tangent) + 1.0)
    along = total(force * unit_tangent)
    spring = stiff_next * length_next - stiff_prev * length_prev
    scale = jnp.where(is_climb, -2.0 * along, spring - along)
    out_ref[:, 0, :] = force + scale * unit_tangent


def neb_project(flags, end_energy, sent, packed, force_rest, before, after, end_positions):
    vmem = pl.BlockSpec(memory_space=pltpu.VMEM)
    smem = pl.BlockSpec(memory_space=pltpu.SMEM)
    return pl.pallas_call(
        project_kernel,
        in_specs=[smem, smem] + [vmem] * 6,
        out_specs=vmem,
        out_shape=jax.ShapeDtypeStruct((3, 1, ATOMS), jnp.float32),
        name="project",
    )(flags, end_energy, sent, packed, force_rest, before, after, end_positions)


def swapped(array, axis, mask):
    pairs = [(i, i ^ mask) for i in range(lax.axis_size(axis))]
    return lax.ppermute(array, axis, pairs)


def summed(array, axis):
    size = lax.axis_size(axis)
    if size & (size - 1):
        return lax.psum(array, axis)
    mask = 1
    while mask < size:
        array = array + swapped(array, axis, mask)
        mask *= 2
    return array


def scattered_rows(rows, axis):
    size = lax.axis_size(axis)
    index = lax.axis_index(axis)
    if size & (size - 1):
        block = rows.shape[0] // size
        return lax.psum_scatter(rows, axis, scatter_dimension=0, tiled=True), index * block
    first = jnp.int32(0)
    mask = 1
    while mask < size:
        half = rows.shape[0] // 2
        bit = (index // mask) % 2
        kept = lax.dynamic_slice_in_dim(rows, bit * half, half, 0)
        sent = lax.dynamic_slice_in_dim(rows, (1 - bit) * half, half, 0)
        rows = kept + swapped(sent, axis, mask)
        first = first + (bit * half).astype(jnp.int32)
        mask *= 2
    return rows, first


def per_device(
    wave_coeffs,
    occupation,
    form_factor,
    g_vectors,
    species,
    proj_count,
    coupling,
    positions,
    energy_rest,
    force_rest,
    end_positions,
    end_energy,
    climb_index,
    tangent_kind,
):
    species_mask, strength = atom_tables(species, proj_count, coupling)
    bands = wave_coeffs.shape[1]
    length = wave_coeffs.shape[3]
    is_live = (jnp.arange(PMAX)[None, :] < proj_count[:, None]).astype(jnp.float32)
    posb = jnp.broadcast_to(positions[0][:, :, None], (3, ATOMS, 128))
    live = jnp.broadcast_to(is_live[:, :, None], (SPECIES, PMAX, 128))
    blk = length // BLOCKS
    half = BLOCKS // 2
    core = lax.axis_index("band") % 2

    def rows_of(first, count):
        part = lax.dynamic_slice_in_dim(wave_coeffs[0], first * blk, count * blk, 2)
        return part.transpose(1, 0, 2).reshape(2 * bands, count * blk)

    chunks = []
    for at, count in CUTS:
        given = rows_of((1 - core) * half + at, count).astype(jnp.float32)
        chunks.append((core * half + at, count, swapped(given, "band", 1)))
    mine = 0.0
    other = 0.0
    for first, count, taken in chunks:
        kept = rows_of(first, count)
        start = first.astype(jnp.int32)[None]
        own_sums, other_sums = contract(
            species, start, [kept, taken], form_factor, g_vectors, posb, live, blk=blk
        )
        mine = mine + own_sums
        other = other + other_sums
    sums = mine + swapped(other, "band", 1)
    proj_sums, first_row = scattered_rows(sums, "ga")
    strength_rows = lax.dynamic_slice_in_dim(
        strength.reshape(ATOMS * PMAX, 1), first_row, proj_sums.shape[0], 0
    )
    packed = nonlocal_terms(proj_sums, first_row, occupation, strength_rows)
    packed = summed(summed(packed, "band"), "ga")
    padded = jnp.concatenate([positions[0], jnp.zeros((1, ATOMS), jnp.float32)], axis=0)
    is_last = lax.broadcasted_iota(jnp.int32, padded.shape, 0) == 3
    sent = jnp.where(is_last, packed + energy_rest, padded)
    before = passed_along(sent, "image", 1)
    after = passed_along(sent, "image", -1)
    image_index = lax.axis_index("image")
    flags = jnp.stack(
        [
            (image_index == 0).astype(jnp.int32),
            (image_index == lax.axis_size("image") - 1).astype(jnp.int32),
            (climb_index[0] == image_index).astype(jnp.int32),
            tangent_kind[0],
        ]
    )
    neb_force = neb_project(
        flags, end_energy, sent, packed, force_rest[0], before, after, end_positions
    )
    return (neb_force.transpose(1, 0, 2), sent[3, :1])


def solution(mesh):
    in_specs = (
        P("image", "band", None, "ga"),
        P("image", "band"),
        P(None, None, "ga"),
        P(None, "ga"),
        P(),
        P(),
        P(),
        P("image", None, None),
        P("image"),
        P("image", None, None),
        P(),
        P(),
        P(),
        P("image"),
    )
    out_specs = (P("image", None, None), P("image"))
    return jax.shard_map(
        per_device, mesh=mesh, in_specs=in_specs, out_specs=out_specs, check_vma=False
    )
```
